32 devices in a mesh: seq: 8 (over z, y), head: 4 (over x, core).
Axes of the slice: x: 2, y: 2, z: 4, core: 2. Of those that a mesh axis runs over, the one named last changes fastest.
Arguments:
- hidden_states: bfloat16 [2048, 1536], P('seq', 'head'), may hold values from -60 to 60
- feature_q: bfloat16 [1536, 384], P(None, 'head'), may hold values from -0.15625 to 0.15625
- feature_k: bfloat16 [1536, 384], P(None, 'head'), may hold values from -0.15625 to 0.15625
- value_w: bfloat16 [1536, 1536], P(None, 'head'), may hold values from -0.15625 to 0.15625
- window_q: bfloat16 [1536, 1536], P(None, 'head'), may hold values from -0.15625 to 0.15625
- window_k: bfloat16 [1536, 1536], P(None, 'head'), may hold values from -0.15625 to 0.15625
- norm_gain: float32 [1536], P('head'), may hold values from 0.5 to 1.5
Outputs:
- mixed: bfloat16 [2048, 1536], P('seq', 'head')
The draws below stay inside these ranges and needn't reach their ends.
All inputs are finite; a program needn't handle non-finite values.
Results may differ from the reference program's by a relative error of at most 0.007.
Values may be sent and summed in bfloat16 or wider, within the bound.
A program may use at most 128 MiB of HBM per device.

```python
import jax
import jax.numpy as jnp
from jax import lax

D = 1536
HEADS = 24
FK = 16
HV = 64
WINDOW_HEAD_SIZE = 64
WIN = 64
TOK_DEV = 256
FEAT = 273
SEQ = 2048


def draw_hidden_states(key, part):
    first = jax.random.fold_in(jax.random.fold_in(key, 17), 0)
    base = jnp.clip(jax.random.normal(first, (SEQ, D), jnp.float32), -6.0, 6.0)
    return base.astype(jnp.bfloat16)


def level_of(rng, dims, shards, least, largest):
    def one(dim, parts):
        draws = jax.random.uniform(jax.random.fold_in(jax.random.fold_in(rng, 6), dim), (parts,), jnp.float32, least / len(shards), largest / len(shards))
        return jnp.repeat(jnp.exp(draws), dims[dim] // parts).reshape((-1,) + (1,) * (len(dims) - dim - 1))

    loudness = one(*shards[0])
    for cut in shards[1:]:
        loudness = loudness * one(*cut)
    return loudness


def bell_draw(stream_key, dims, deviation, reach, cuts=(), kind=jnp.bfloat16):
    drawn = jax.random.normal(stream_key, dims, jnp.float32) * deviation
    if len(cuts) > 0:
        drawn = level_of(stream_key, dims, cuts, -0.22, 0.18) * drawn
    return jnp.clip(drawn, min=-reach, max=reach).astype(kind)


def setup_inputs(seed: int = 0) -> dict:
    splits = jax.random.split(jax.random.key(seed), 8)
    return {
        "hidden_states": draw_hidden_states(jax.random.fold_in(splits[7], 71), 0),
        "feature_q": bell_draw(splits[1], (D, HEADS * FK), D ** -0.5, 0.15625, ((1, 4),)),
        "feature_k": bell_draw(splits[2], (D, HEADS * FK), D ** -0.5, 0.15625, ((1, 4),)),
        "value_w": bell_draw(splits[3], (D, HEADS * HV), D ** -0.5, 0.15625, ((1, 4),)),
        "window_q": bell_draw(splits[4], (D, HEADS * WINDOW_HEAD_SIZE), D ** -0.5, 0.15625, ((1, 4),)),
        "window_k": bell_draw(splits[5], (D, HEADS * WINDOW_HEAD_SIZE), D ** -0.5, 0.15625, ((1, 4),)),
        "norm_gain": jnp.clip(1.0 + 0.1 * jax.random.normal(splits[6], (HEADS * HV,), jnp.float32), 0.5, 1.5),
    }


HIGH_ACCURACY = lax.Precision.HIGHEST

def expand(x):
    lead = x.shape[:-1]
    width = x.shape[-1]
    ones = jnp.ones(lead + (1,), jnp.float32)
    quad = (x[..., :, None] * x[..., None, :]).reshape(lead + (width * width,)) * 0.5 ** 0.5
    return jnp.concatenate([ones, x, quad], axis=-1)

def reference(hidden_states, feature_q, feature_k, value_w, window_q, window_k, norm_gain):
    count = SEQ // TOK_DEV
    blocks = hidden_states.reshape(count, TOK_DEV, D)
    order = jnp.arange(count, dtype=jnp.int32)

    def step(carry, item):
        state, prev_keys, prev_values = carry
        block, index = item
        offset = index * TOK_DEV
        query = (jnp.dot(block, feature_q, preferred_element_type=jnp.float32) * FK ** (-0.25)).reshape(TOK_DEV, HEADS, FK)
        key = (jnp.dot(block, feature_k, preferred_element_type=jnp.float32) * FK ** (-0.25)).reshape(TOK_DEV, HEADS, FK)
        values = jnp.dot(block, value_w, preferred_element_type=jnp.float32).astype(jnp.bfloat16)
        wquery = jnp.dot(block, window_q, preferred_element_type=jnp.float32).astype(jnp.bfloat16)
        wkey = jnp.dot(block, window_k, preferred_element_type=jnp.float32).astype(jnp.bfloat16)
        value3 = values.reshape(TOK_DEV, HEADS, HV).astype(jnp.float32)
        inner = jnp.einsum('lhf,mhf->hlm', query, key, precision=HIGH_ACCURACY)
        kernel = 1.0 + inner + 0.5 * inner * inner
        rows_i = jnp.arange(TOK_DEV, dtype=jnp.int32)
        causal = rows_i[:, None] >= rows_i[None, :]
        kernel = jnp.where(causal[None], kernel, 0.0).astype(jnp.bfloat16)
        intra = jnp.einsum('hlm,mhv->lhv', kernel.astype(jnp.float32), value3, precision=HIGH_ACCURACY)
        phi_q = expand(query)
        phi_k = expand(key)
        cross = jnp.einsum('lhf,fhv->lhv', phi_q, state, precision=HIGH_ACCURACY)
        linear = intra + cross
        scale = lax.rsqrt(lax.optimization_barrier(jnp.mean(linear * linear, axis=-1, keepdims=True)) + 1e-05)
        normed = linear * scale * norm_gain.reshape(HEADS, HV)
        key_rows_full = jnp.concatenate([prev_keys, wkey], axis=0).reshape(TOK_DEV + WIN, HEADS, WINDOW_HEAD_SIZE).astype(jnp.float32)
        values_all = jnp.concatenate([prev_values, values], axis=0).reshape(TOK_DEV + WIN, HEADS, HV).astype(jnp.float32)
        query_weight3 = wquery.reshape(TOK_DEV, HEADS, WINDOW_HEAD_SIZE).astype(jnp.float32)
        window_logits = jnp.einsum('qxo,bxo->xqb', query_weight3, key_rows_full, precision=HIGH_ACCURACY) * WINDOW_HEAD_SIZE ** (-0.5)
        query_pos = offset + rows_i[:, None]
        key_pos = offset - WIN + jnp.arange(TOK_DEV + WIN, dtype=jnp.int32)[None, :]
        valid = (key_pos <= query_pos) & (key_pos > query_pos - WIN) & (key_pos >= 0)
        window_logits = jnp.where(valid[None], window_logits, -1e+30)
        top = lax.optimization_barrier(jnp.max(window_logits, axis=-1, keepdims=True))
        expw = jnp.exp(window_logits - top)
        weights = (expw / lax.optimization_barrier(jnp.sum(expw, axis=-1, keepdims=True))).astype(jnp.bfloat16)
        window = jnp.einsum('hlm,mhv->lhv', weights.astype(jnp.float32), values_all, precision=HIGH_ACCURACY)
        mixed = (normed + window).astype(jnp.bfloat16).reshape(TOK_DEV, HEADS * HV)
        new_state = state + jnp.einsum('lhf,lhv->fhv', phi_k, value3, precision=HIGH_ACCURACY)
        return ((new_state, wkey[TOK_DEV - WIN:], values[TOK_DEV - WIN:]), mixed)
    init = (jnp.zeros((FEAT, HEADS, HV), jnp.float32), jnp.zeros((WIN, HEADS * WINDOW_HEAD_SIZE), jnp.bfloat16), jnp.zeros((WIN, HEADS * HV), jnp.bfloat16))
    carry, outputs = lax.scan(step, init, (blocks, order))
    return outputs.reshape(SEQ, HEADS * HV)
```

```python
import functools

import jax
import jax.numpy as jnp
import numpy as np
from jax import lax
from jax.experimental import pallas as pl
from jax.experimental.pallas import tpu as pltpu
from jax.sharding import PartitionSpec as P

FK = 16
HV = 64
WIN = 64
LANES = 128
CHUNK = 256
MESH = pl.DeviceIdType.MESH
F32 = jnp.float32
BF16 = jnp.bfloat16


def features(heads):
    upper, lower = np.triu_indices(FK)
    one = heads * FK
    left, right, owner, weight = [], [], [], []
    for head in range(heads):
        base = head * FK
        left += [one] + [base + i for i in range(FK)] + [base + i for i in upper]
        right += [one] + [one] * FK + [base + j for j in lower]
        owner += [head] * (1 + FK + len(upper))
        weight += [1.0] * (1 + FK) + [0.5 if i == j else 1.0 for i, j in zip(upper, lower)]
    count = len(left)
    width = -(-count // CHUNK) * CHUNK
    ea = np.zeros((2 * LANES, width), np.float32)
    eb = np.zeros((2 * LANES, width), np.float32)
    mask = np.zeros((-(-heads // 8) * 8, width), np.float32)
    for lane in range(count):
        ea[[left[lane], LANES + left[lane]], lane] = 1.0
        eb[[right[lane], LANES + right[lane]], lane] = 1.0
        mask[owner[lane], lane] = weight[lane]
    return ea, eb, mask


def dot(a, b):
    return jnp.dot(a, b, preferred_element_type=F32)


def dot_t(a, b):
    return lax.dot_general(a, b, (((1,), (1,)), ((), ())), preferred_element_type=F32)


def split(x):
    high = x.astype(BF16)
    return high, (x - high.astype(F32)).astype(BF16)


def kernel(blocks, group, heads, wire, hid, fq, fk, vw, wqw, wkw, gain, ea, eb, mask, out,
           hbuf, fq_v, fk_v, vw_v, wq_v, wk_v, gain_v, ea_v, eb_v, mask_v,
           q_acc, k_acc, v_acc, wq_acc, wk_acc, v_b, wq_b, wk_b, halo_out, halo_in,
           phi_q, local, y_out, y_in, z_out, z_in, lin, win,
           load_sem, g_send, g_recv, h_send, h_recv, y_send, y_recv, z_send, z_recv):
    s, h = lax.axis_index("seq"), lax.axis_index("head")
    rows, depth = hid.shape
    chunks = local.shape[0]
    pair, inner = s // 2, s % 2
    last_pair = blocks // 2 - 1
    pairs = heads // 2

    loads = [
        pltpu.make_async_copy(src, dst, load_sem.at[i])
        for i, (src, dst) in enumerate((
            (hid, hbuf.at[h]), (fk, fk_v), (vw, vw_v), (wkw, wk_v), (fq, fq_v), (wqw, wq_v),
            (ea, ea_v), (eb, eb_v), (mask, mask_v), (gain, gain_v),
        ))
    ]
    for load in loads:
        load.start()

    barrier = pltpu.get_barrier_semaphore()
    bits = []
    bit = group // 2
    while bit:
        bits.append(bit)
        bit //= 2

    def flip(value, by):
        return value + by - 2 * by * ((value // by) % 2)

    for by in bits:
        pl.semaphore_signal(barrier, inc=1, device_id=(s, flip(h, by)), device_id_type=MESH)
    expected = len(bits)
    for by in (1, -1, 2, -2):
        there = s + by
        valid = jnp.logical_and(there >= 0, there < blocks)

        @pl.when(valid)
        def _(there=there):
            pl.semaphore_signal(barrier, inc=1, device_id=(there, h), device_id_type=MESH)

        expected = expected + jnp.where(valid, 1, 0)

    lane = lax.broadcasted_iota(jnp.int32, (rows, LANES), 1)
    fill = jnp.where(lane >= heads * FK, FK**0.25, 0.0).astype(F32)
    q_acc[...] = fill
    k_acc[...] = fill
    pl.semaphore_wait(barrier, expected)
    loads[0].wait()

    moves = {}

    def send_block(index, owner, by):
        move = pltpu.make_async_remote_copy(
            src_ref=hbuf.at[owner], dst_ref=hbuf.at[owner],
            send_sem=g_send.at[index], recv_sem=g_recv.at[index],
            device_id=(s, flip(h, by)), device_id_type=MESH,
        )
        move.start()
        return move

    plan = []

    def spread(owner_flip, from_level):
        for level in range(from_level, len(bits)):
            plan.append((owner_flip, level))
            spread(owner_flip ^ bits[level], level + 1)

    spread(0, 0)
    arrives = {}
    for index, (own, level) in enumerate(plan):
        arrives[own ^ bits[level]] = index

    def owner_of(mask_bits):
        value = h
        for by in bits:
            if mask_bits & by:
                value = flip(value, by)
        return value

    def forward(block):
        for index, (own, level) in enumerate(plan):
            if own == block:
                moves[index] = send_block(index, owner_of(block), bits[level])

    def arrive(block):
        moves_index = arrives[block]
        moves[moves_index].wait_recv()

    def part(weight, owner):
        return weight[pl.ds(pl.multiple_of(owner * depth, depth), depth), :]

    def part_t(weight, owner):
        return weight[:, pl.ds(pl.multiple_of(owner * depth, depth), depth)]

    forward(0)
    sequence = sorted(range(1, group), key=lambda b: (b.bit_length(), b))
    main = ((v_acc, vw_v), (wk_acc, wk_v), (wq_acc, wq_v))
    small = ((k_acc, fk_v), (q_acc, fq_v))
    for load in loads[1:6]:
        load.wait()
    for position, block in enumerate([0] + sequence):
        if block:
            arrive(block)
            forward(block)
        owner = owner_of(block)
        tile = hbuf[owner]
        final = position == group - 1
        for acc, weight in small:
            if final and acc is q_acc:
                continue
            acc[:, : heads * FK] += dot_t(tile, part_t(weight, owner))
        for acc, weight in main:
            if final and acc is wq_acc:
                continue
            product = dot(tile, part(weight, owner))
            acc[...] = product if position == 0 else acc[...] + product
    last_tile, last_owner = tile, owner

    v_b[...] = v_acc[...].astype(BF16)
    wk_b[...] = wk_acc[...].astype(BF16)
    width = heads * HV
    halo_out[:, :width] = wk_b[rows - WIN :, :]
    halo_out[:, width:] = v_b[rows - WIN :, :]
    after = lax.rem(s + 1, blocks)
    halo = pltpu.make_async_remote_copy(
        src_ref=halo_out, dst_ref=halo_in, send_sem=h_send, recv_sem=h_recv,
        device_id=(after, h), device_id_type=MESH,
    )

    @pl.when(s < blocks - 1)
    def _():
        halo.start()

    for load in loads[6:]:
        load.wait()

    k_high, k_low = split(k_acc[...] * FK**-0.25)
    k_cat = jnp.concatenate([k_high, k_low], axis=1)
    v_turned = v_b[...].T
    exchange = []
    for c in range(chunks):
        lanes = slice(c * CHUNK, (c + 1) * CHUNK)
        phi_k = (dot(k_cat, ea_v[:, lanes]) * dot(k_cat, eb_v[:, lanes])).astype(BF16)
        full = dot(v_turned, phi_k)
        state = full[:HV] * mask_v[0:1, lanes]
        for head in range(1, heads):
            state += full[head * HV : (head + 1) * HV] * mask_v[head : head + 1, lanes]
        local[c] = state
        y_out[c] = state.astype(wire)
        move = pltpu.make_async_remote_copy(
            src_ref=y_out.at[c], dst_ref=y_in.at[c], send_sem=y_send.at[c], recv_sem=y_recv.at[c],
            device_id=(flip(s, 1), h), device_id_type=MESH,
        )
        move.start()
        exchange.append(move)
    beyond = lax.rem(s + 2, blocks)
    chain = [
        pltpu.make_async_remote_copy(
            src_ref=z_out.at[c], dst_ref=z_in.at[c], send_sem=z_send.at[c], recv_sem=z_recv.at[c],
            device_id=(beyond, h), device_id_type=MESH,
        )
        for c in range(chunks)
    ]

    q_acc[:, : heads * FK] += dot_t(last_tile, part_t(fq_v, last_owner))
    wq_b[...] = (wq_acc[...] + dot(last_tile, part(wq_v, last_owner))).astype(BF16)
    q_high, q_low = split(q_acc[...] * FK**-0.25)
    q_cat = jnp.concatenate([q_high, q_low], axis=1)

    def features_q():
        for c in range(chunks):
            lanes = slice(c * CHUNK, (c + 1) * CHUNK)
            phi_q[:, lanes] = (dot(q_cat, ea_v[:, lanes]) * dot(q_cat, eb_v[:, lanes])).astype(BF16)

    k_twice = jnp.concatenate([k_high, k_high], axis=1)
    half = rows // 2
    lane_q = lax.broadcasted_iota(jnp.int32, (half, 2 * LANES), 1) % LANES // FK
    low_half = lax.broadcasted_iota(jnp.int32, (half, LANES), 1) < HV

    def intra(p, block):
        rs = slice(block * half, (block + 1) * half)
        keys = (block + 1) * half
        qs = q_cat[rs]
        stacked = jnp.concatenate(
            [jnp.where(lane_q == 2 * p, qs, 0), jnp.where(lane_q == 2 * p + 1, qs, 0)], axis=0
        )
        a = dot_t(stacked, k_twice[:keys]) + dot_t(stacked[:, :LANES], k_low[:keys])
        kern = 1.0 + a + 0.5 * a * a
        row = lax.broadcasted_iota(jnp.int32, a.shape, 0) % half + block * half
        col = lax.broadcasted_iota(jnp.int32, a.shape, 1)
        kern = jnp.where(row >= col, kern, 0.0).astype(BF16)
        both = dot(kern, v_b[:keys, p * LANES : (p + 1) * LANES])
        lin[rs, p * LANES : (p + 1) * LANES] = jnp.where(low_half, both[:half], both[half:])

    low_win = lax.broadcasted_iota(jnp.int32, (WIN, LANES), 1) < HV
    row_w = lax.broadcasted_iota(jnp.int32, (2 * WIN, 2 * WIN), 0) % WIN
    col_w = lax.broadcasted_iota(jnp.int32, (2 * WIN, 2 * WIN), 1)
    seen = jnp.logical_and(col_w > row_w, col_w <= row_w + WIN)

    def window(p, block):
        ls = slice(p * LANES, (p + 1) * LANES)
        qs = wq_b[block * WIN : (block + 1) * WIN, ls]
        stacked = jnp.concatenate([jnp.where(low_win, qs, 0), jnp.where(low_win, 0, qs)], axis=0)
        valid = seen
        if block == 0:
            keys = jnp.concatenate([halo_in[:, ls], wk_b[:WIN, ls]], axis=0)
            vals = jnp.concatenate(
                [halo_in[:, width + p * LANES : width + (p + 1) * LANES], v_b[:WIN, ls]], axis=0
            )
            valid = jnp.logical_and(seen, jnp.logical_or(col_w >= WIN, s > 0))
        else:
            keys = wk_b[(block - 1) * WIN : (block + 1) * WIN, ls]
            vals = v_b[(block - 1) * WIN : (block + 1) * WIN, ls]
        logits = jnp.where(valid, dot_t(stacked, keys) * HV**-0.5, -1e30)
        expw = jnp.exp(logits - jnp.max(logits, axis=-1, keepdims=True))
        weights = (expw / jnp.sum(expw, axis=-1, keepdims=True)).astype(BF16)
        both = dot(weights, vals)
        win[block * WIN : (block + 1) * WIN, ls] = jnp.where(low_win, both[:WIN], both[WIN:])

    for p in range(pairs):
        for block in range(2):
            intra(p, block)

    for c in range(chunks):
        exchange[c].wait_recv()

        @pl.when(pair == 0)
        def _(c=c):
            z_out[c] = (local[c] + y_in[c].astype(F32)).astype(wire)
            z_in[c] = jnp.zeros_like(z_in[c])

            @pl.when(pair < last_pair)
            def _():
                chain[c].start()

    features_q()
    for p in range(pairs):
        for block in range(1, rows // WIN):
            window(p, block)

    @pl.when(s > 0)
    def _():
        halo.wait_recv()

    @pl.when(s == 0)
    def _():
        halo_in[...] = jnp.zeros_like(halo_in)

    for p in range(pairs):
        window(p, 0)

    mine = jnp.where(inner == 1, 1.0, 0.0).astype(F32)
    total = None
    for c in range(chunks):
        lanes = slice(c * CHUNK, (c + 1) * CHUNK)

        @pl.when(pair > 0)
        def _(c=c):
            chain[c].wait_recv()

            @pl.when(pair < last_pair)
            def _():
                z_out[c] = (z_in[c].astype(F32) + (local[c] + y_in[c].astype(F32))).astype(wire)
                chain[c].start()

        earlier = z_in[c].astype(F32) + mine * y_in[c].astype(F32)
        big = jnp.concatenate(
            [
                jnp.where(mask_v[head : head + 1, lanes] > 0, earlier, 0.0).astype(BF16)
                for head in range(heads)
            ],
            axis=0,
        )
        product = dot_t(phi_q[:, lanes], big)
        if c == 0:
            lin[...] += product
        else:
            lin[...] += product

    ones = jnp.where(
        lax.broadcasted_iota(jnp.int32, (2 * LANES, LANES), 0) % LANES // HV
        == lax.broadcasted_iota(jnp.int32, (2 * LANES, LANES), 1) // HV,
        1.0,
        0.0,
    ).astype(BF16)
    for p in range(pairs):
        ls = slice(p * LANES, (p + 1) * LANES)
        linear = lin[:, ls]
        high, low = split(linear * linear)
        mean = dot(jnp.concatenate([high, low], axis=1), ones) * (1.0 / HV)
        normed = linear * lax.rsqrt(mean + 1e-05) * gain_v[:, ls]
        out[:, ls] = (normed + win[:, ls]).astype(BF16)

    for move in moves.values():
        move.wait_send()
    for move in exchange:
        move.wait_send()

    @pl.when(s < blocks - 1)
    def _():
        halo.wait_send()

    @pl.when(pair < last_pair)
    def _():
        for move in chain:
            move.wait_send()


def solution(mesh):
    blocks, group = mesh.shape["seq"], mesh.shape["head"]

    def body(hidden_states, feature_q, feature_k, value_w, window_q, window_k, norm_gain):
        rows, depth = hidden_states.shape
        heads = feature_q.shape[1] // FK
        full, width = value_w.shape
        ea, eb, mask = features(heads)
        feats = ea.shape[1]
        chunks = feats // CHUNK
        wire = BF16 if blocks <= 16 else F32
        dma, anywhere = pltpu.SemaphoreType.DMA, pl.BlockSpec(memory_space=pl.ANY)
        state = (chunks, HV, CHUNK)
        return pl.pallas_call(
            functools.partial(kernel, blocks, group, heads, wire),
            out_shape=jax.ShapeDtypeStruct((rows, width), BF16),
            in_specs=[anywhere] * 10,
            out_specs=pl.BlockSpec(memory_space=pltpu.VMEM),
            scratch_shapes=[
                pltpu.VMEM((group, rows, depth), BF16),
                pltpu.VMEM((heads * FK, full), BF16),
                pltpu.VMEM((heads * FK, full), BF16),
                pltpu.VMEM((full, width), BF16),
                pltpu.VMEM((full, width), BF16),
                pltpu.VMEM((full, width), BF16),
                pltpu.VMEM((1, width), F32),
                pltpu.VMEM(ea.shape, BF16),
                pltpu.VMEM(eb.shape, BF16),
                pltpu.VMEM(mask.shape, F32),
                pltpu.VMEM((rows, LANES), F32),
                pltpu.VMEM((rows, LANES), F32),
                pltpu.VMEM((rows, width), F32),
                pltpu.VMEM((rows, width), F32),
                pltpu.VMEM((rows, width), F32),
                pltpu.VMEM((rows, width), BF16),
                pltpu.VMEM((rows, width), BF16),
                pltpu.VMEM((rows, width), BF16),
                pltpu.VMEM((WIN, 2 * width), BF16),
                pltpu.VMEM((WIN, 2 * width), BF16),
                pltpu.VMEM((rows, feats), BF16),
                pltpu.VMEM(state, F32),
                pltpu.VMEM(state, wire),
                pltpu.VMEM(state, wire),
                pltpu.VMEM(state, wire),
                pltpu.VMEM(state, wire),
                pltpu.VMEM((rows, width), F32),
                pltpu.VMEM((rows, width), F32),
                dma((10,)),
                dma((group - 1,)),
                dma((group - 1,)),
                dma,
                dma,
                dma((chunks,)),
                dma((chunks,)),
                dma((chunks,)),
                dma((chunks,)),
            ],
            compiler_params=pltpu.CompilerParams(
                collective_id=0, has_side_effects=True, vmem_limit_bytes=66_000_000
            ),
            name="based_layer",
        )(
            hidden_states, feature_q.T, feature_k.T, value_w, window_q, window_k,
            norm_gain.reshape(1, width), jnp.asarray(ea, BF16), jnp.asarray(eb, BF16),
            jnp.asarray(mask, F32),
        )

    return jax.shard_map(
        body,
        mesh=mesh,
        in_specs=(P("seq", "head"),) + (P(None, "head"),) * 5 + (P("head"),),
        out_specs=P("seq", "head"),
        check_vma=False,
    )
```

```python
import functools

import jax
import jax.numpy as jnp
import numpy as np
from jax import lax
from jax.experimental import pallas as pl
from jax.experimental.pallas import tpu as pltpu
from jax.sharding import PartitionSpec as P

FK = 16
HV = 64
WIN = 64
LANES = 128
CHUNK = 128
WIDE = 256
MESH = pl.DeviceIdType.MESH
F32 = jnp.float32
BF16 = jnp.bfloat16


def features(heads):
    upper, lower = np.triu_indices(FK)
    one = heads * FK
    left, right, owner, weight = [], [], [], []
    for head in range(heads):
        base = head * FK
        left += [one] + [base + i for i in range(FK)] + [base + i for i in upper]
        right += [one] + [one] * FK + [base + j for j in lower]
        owner += [head] * (1 + FK + len(upper))
        weight += [1.0] * (1 + FK) + [0.5 if i == j else 1.0 for i, j in zip(upper, lower)]
    count = len(left)
    width = -(-count // WIDE) * WIDE
    ea = np.zeros((2 * LANES, width), np.float32)
    eb = np.zeros((2 * LANES, width), np.float32)
    mask = np.zeros((-(-heads // 8) * 8, width), np.float32)
    for lane in range(count):
        ea[[left[lane], LANES + left[lane]], lane] = 1.0
        eb[[right[lane], LANES + right[lane]], lane] = 1.0
        mask[owner[lane], lane] = weight[lane]
    return ea, eb, mask


def dot(a, b):
    return jnp.dot(a, b, preferred_element_type=F32)


def dot_t(a, b):
    return lax.dot_general(a, b, (((1,), (1,)), ((), ())), preferred_element_type=F32)


def split(x):
    high = x.astype(BF16)
    return high, (x - high.astype(F32)).astype(BF16)


def kernel(blocks, group, heads, wire, hid, fq, fk, vw, wqw, wkw, gain, ea, eb, mask, out,
           hbuf, fq_v, fk_v, vw_v, wq_v, wk_v, gain_v, ea_v, eb_v, mask_v,
           q_acc, k_acc, v_acc, wq_acc, wk_acc, v_b, wq_b, wk_b, halo_out, halo_in,
           phi_q, local, y_out, y_in, z_out, z_in, lin, win,
           load_sem, g_send, g_recv, h_send, h_recv, y_send, y_recv, z_send, z_recv):
    s, h = lax.axis_index("seq"), lax.axis_index("head")
    rows, depth = hid.shape
    chunks = local.shape[0]
    pair, inner = s // 2, s % 2
    last_pair = blocks // 2 - 1
    pairs = heads // 2

    loads = [
        pltpu.make_async_copy(src, dst, load_sem.at[i])
        for i, (src, dst) in enumerate((
            (hid, hbuf.at[h]), (fk, fk_v), (vw, vw_v), (wkw, wk_v), (fq, fq_v), (wqw, wq_v),
            (ea, ea_v), (eb, eb_v), (mask, mask_v), (gain, gain_v),
        ))
    ]
    for load in loads:
        load.start()

    barrier = pltpu.get_barrier_semaphore()
    bits = []
    bit = group // 2
    while bit:
        bits.append(bit)
        bit //= 2

    def flip(value, by):
        return value + by - 2 * by * ((value // by) % 2)

    for by in bits:
        pl.semaphore_signal(barrier, inc=1, device_id=(s, flip(h, by)), device_id_type=MESH)
    expected = len(bits)
    for by in (1, -1, 2, -2):
        there = s + by
        valid = jnp.logical_and(there >= 0, there < blocks)

        @pl.when(valid)
        def _(there=there):
            pl.semaphore_signal(barrier, inc=1, device_id=(there, h), device_id_type=MESH)

        expected = expected + jnp.where(valid, 1, 0)

    lane = lax.broadcasted_iota(jnp.int32, (rows, LANES), 1)
    fill = jnp.where(lane >= heads * FK, FK**0.25, 0.0).astype(F32)
    q_acc[...] = fill
    k_acc[...] = fill
    pl.semaphore_wait(barrier, expected)
    loads[0].wait()

    moves = {}

    def send_block(index, owner, by):
        move = pltpu.make_async_remote_copy(
            src_ref=hbuf.at[owner], dst_ref=hbuf.at[owner],
            send_sem=g_send.at[index], recv_sem=g_recv.at[index],
            device_id=(s, flip(h, by)), device_id_type=MESH,
        )
        move.start()
        return move

    plan = []

    def spread(owner_flip, from_level):
        for level in range(from_level, len(bits)):
            plan.append((owner_flip, level))
            spread(owner_flip ^ bits[level], level + 1)

    spread(0, 0)
    arrives = {}
    for index, (own, level) in enumerate(plan):
        arrives[own ^ bits[level]] = index

    def owner_of(mask_bits):
        value = h
        for by in bits:
            if mask_bits & by:
                value = flip(value, by)
        return value

    def forward(block):
        for index, (own, level) in enumerate(plan):
            if own == block:
                moves[index] = send_block(index, owner_of(block), bits[level])

    def arrive(block):
        moves_index = arrives[block]
        moves[moves_index].wait_recv()

    def part(weight, owner):
        return weight[pl.ds(pl.multiple_of(owner * depth, depth), depth), :]

    def part_t(weight, owner):
        return weight[:, pl.ds(pl.multiple_of(owner * depth, depth), depth)]

    forward(0)
    sequence = sorted(range(1, group), key=lambda b: (b.bit_length(), b))
    main = ((v_acc, vw_v), (wk_acc, wk_v), (wq_acc, wq_v))
    small = ((k_acc, fk_v), (q_acc, fq_v))
    for load in loads[1:6]:
        load.wait()
    for position, block in enumerate([0] + sequence):
        if block:
            arrive(block)
            forward(block)
        owner = owner_of(block)
        tile = hbuf[owner]
        final = position == group - 1
        for acc, weight in small:
            if final and acc is q_acc:
                continue
            acc[:, : heads * FK] += dot_t(tile, part_t(weight, owner))
        for acc, weight in main:
            if final and acc is not v_acc:
                continue
            product = dot(tile, part(weight, owner))
            acc[...] = product if position == 0 else acc[...] + product
    last_tile, last_owner = tile, owner

    v_b[...] = v_acc[...].astype(BF16)
    for load in loads[6:]:
        load.wait()

    k_high, k_low = split(k_acc[...] * FK**-0.25)
    k_cat = jnp.concatenate([k_high, k_low], axis=1)
    v_turned = v_b[...].T
    exchange = []
    for wide in range(chunks * CHUNK // WIDE):
        lanes = slice(wide * WIDE, (wide + 1) * WIDE)
        phi_k = (dot(k_cat, ea_v[:, lanes]) * dot(k_cat, eb_v[:, lanes])).astype(BF16)
        full = dot(v_turned, phi_k)
        state = full[:HV] * mask_v[0:1, lanes]
        for head in range(1, heads):
            state += full[head * HV : (head + 1) * HV] * mask_v[head : head + 1, lanes]
        for piece in range(WIDE // CHUNK):
            c = wide * (WIDE // CHUNK) + piece
            part_state = state[:, piece * CHUNK : (piece + 1) * CHUNK]
            local[c] = part_state
            y_out[c] = part_state.astype(wire)
            move = pltpu.make_async_remote_copy(
                src_ref=y_out.at[c], dst_ref=y_in.at[c],
                send_sem=y_send.at[c], recv_sem=y_recv.at[c],
                device_id=(flip(s, 1), h), device_id_type=MESH,
            )
            move.start()
            exchange.append(move)
    beyond = lax.rem(s + 2, blocks)
    chain = [
        pltpu.make_async_remote_copy(
            src_ref=z_out.at[c], dst_ref=z_in.at[c], send_sem=z_send.at[c], recv_sem=z_recv.at[c],
            device_id=(beyond, h), device_id_type=MESH,
        )
        for c in range(chunks)
    ]

    wk_b[...] = (wk_acc[...] + dot(last_tile, part(wk_v, last_owner))).astype(BF16)
    width = heads * HV
    halo_out[:, :width] = wk_b[rows - WIN :, :]
    halo_out[:, width:] = v_b[rows - WIN :, :]
    after = lax.rem(s + 1, blocks)
    halo = pltpu.make_async_remote_copy(
        src_ref=halo_out, dst_ref=halo_in, send_sem=h_send, recv_sem=h_recv,
        device_id=(after, h), device_id_type=MESH,
    )

    late = jnp.logical_and(pair == 0, inner == 1)

    @pl.when(jnp.logical_and(s < blocks - 1, jnp.logical_not(late)))
    def _():
        halo.start()

    q_acc[:, : heads * FK] += dot_t(last_tile, part_t(fq_v, last_owner))
    wq_b[...] = (wq_acc[...] + dot(last_tile, part(wq_v, last_owner))).astype(BF16)
    q_high, q_low = split(q_acc[...] * FK**-0.25)
    q_cat = jnp.concatenate([q_high, q_low], axis=1)

    def features_q():
        for wide in range(chunks * CHUNK // WIDE):
            lanes = slice(wide * WIDE, (wide + 1) * WIDE)
            phi_q[:, lanes] = (dot(q_cat, ea_v[:, lanes]) * dot(q_cat, eb_v[:, lanes])).astype(BF16)

    k_twice = jnp.concatenate([k_high, k_high], axis=1)
    half = rows // 2
    lane_q = lax.broadcasted_iota(jnp.int32, (half, 2 * LANES), 1) % LANES // FK
    low_half = lax.broadcasted_iota(jnp.int32, (half, LANES), 1) < HV

    def intra(p, block):
        rs = slice(block * half, (block + 1) * half)
        keys = (block + 1) * half
        qs = q_cat[rs]
        stacked = jnp.concatenate(
            [jnp.where(lane_q == 2 * p, qs, 0), jnp.where(lane_q == 2 * p + 1, qs, 0)], axis=0
        )
        a = dot_t(stacked, k_twice[:keys]) + dot_t(stacked[:, :LANES], k_low[:keys])
        kern = 1.0 + a + 0.5 * a * a
        row = lax.broadcasted_iota(jnp.int32, a.shape, 0) % half + block * half
        col = lax.broadcasted_iota(jnp.int32, a.shape, 1)
        kern = jnp.where(row >= col, kern, 0.0).astype(BF16)
        both = dot(kern, v_b[:keys, p * LANES : (p + 1) * LANES])
        lin[rs, p * LANES : (p + 1) * LANES] = jnp.where(low_half, both[:half], both[half:])

    low_win = lax.broadcasted_iota(jnp.int32, (WIN, LANES), 1) < HV
    row_w = lax.broadcasted_iota(jnp.int32, (2 * WIN, 2 * WIN), 0) % WIN
    col_w = lax.broadcasted_iota(jnp.int32, (2 * WIN, 2 * WIN), 1)
    seen = jnp.logical_and(col_w > row_w, col_w <= row_w + WIN)

    def window(p, block):
        ls = slice(p * LANES, (p + 1) * LANES)
        qs = wq_b[block * WIN : (block + 1) * WIN, ls]
        stacked = jnp.concatenate([jnp.where(low_win, qs, 0), jnp.where(low_win, 0, qs)], axis=0)
        valid = seen
        if block == 0:
            keys = jnp.concatenate([halo_in[:, ls], wk_b[:WIN, ls]], axis=0)
            vals = jnp.concatenate(
                [halo_in[:, width + p * LANES : width + (p + 1) * LANES], v_b[:WIN, ls]], axis=0
            )
            valid = jnp.logical_and(seen, jnp.logical_or(col_w >= WIN, s > 0))
        else:
            keys = wk_b[(block - 1) * WIN : (block + 1) * WIN, ls]
            vals = v_b[(block - 1) * WIN : (block + 1) * WIN, ls]
        logits = jnp.where(valid, dot_t(stacked, keys) * HV**-0.5, -1e30)
        expw = jnp.exp(logits - jnp.max(logits, axis=-1, keepdims=True))
        weights = (expw / jnp.sum(expw, axis=-1, keepdims=True)).astype(BF16)
        both = dot(weights, vals)
        win[block * WIN : (block + 1) * WIN, ls] = jnp.where(low_win, both[:WIN], both[WIN:])

    for p in range(pairs):
        for block in range(2):
            intra(p, block)

    for c in range(chunks):
        exchange[c].wait_recv()

        @pl.when(pair == 0)
        def _(c=c):
            z_out[c] = (local[c] + y_in[c].astype(F32)).astype(wire)
            z_in[c] = jnp.zeros_like(z_in[c])

            @pl.when(pair < last_pair)
            def _():
                chain[c].start()

    @pl.when(jnp.logical_and(s < blocks - 1, late))
    def _():
        halo.start()

    def relay(c):
        chain[c].wait_recv()

        @pl.when(pair < last_pair)
        def _():
            z_out[c] = (z_in[c].astype(F32) + (local[c] + y_in[c].astype(F32))).astype(wire)
            chain[c].start()

    @pl.when(pair == 1)
    def _():
        for c in range(chunks):
            relay(c)

    features_q()
    for p in range(pairs):
        for block in range(1, rows // WIN):
            window(p, block)

    @pl.when(s > 0)
    def _():
        halo.wait_recv()

    @pl.when(s == 0)
    def _():
        halo_in[...] = jnp.zeros_like(halo_in)

    for p in range(pairs):
        window(p, 0)

    mine = jnp.where(inner == 1, 1.0, 0.0).astype(F32)
    for wide in range(chunks * CHUNK // WIDE):
        lanes = slice(wide * WIDE, (wide + 1) * WIDE)
        pieces = range(wide * (WIDE // CHUNK), (wide + 1) * (WIDE // CHUNK))

        @pl.when(pair > 1)
        def _(pieces=pieces):
            for c in pieces:
                relay(c)

        earlier = jnp.concatenate(
            [z_in[c].astype(F32) + mine * y_in[c].astype(F32) for c in pieces], axis=1
        )
        big = jnp.concatenate(
            [
                jnp.where(mask_v[head : head + 1, lanes] > 0, earlier, 0.0).astype(BF16)
                for head in range(heads)
            ],
            axis=0,
        )
        lin[...] += dot_t(phi_q[:, lanes], big)

    ones = jnp.where(
        lax.broadcasted_iota(jnp.int32, (2 * LANES, LANES), 0) % LANES // HV
        == lax.broadcasted_iota(jnp.int32, (2 * LANES, LANES), 1) // HV,
        1.0,
        0.0,
    ).astype(BF16)
    for p in range(pairs):
        ls = slice(p * LANES, (p + 1) * LANES)
        linear = lin[:, ls]
        high, low = split(linear * linear)
        mean = dot(jnp.concatenate([high, low], axis=1), ones) * (1.0 / HV)
        normed = linear * lax.rsqrt(mean + 1e-05) * gain_v[ls].reshape(1, LANES)
        out[:, ls] = (normed + win[:, ls]).astype(BF16)

    for move in moves.values():
        move.wait_send()
    for move in exchange:
        move.wait_send()

    @pl.when(s < blocks - 1)
    def _():
        halo.wait_send()

    @pl.when(pair < last_pair)
    def _():
        for move in chain:
            move.wait_send()


def solution(mesh):
    blocks, group = mesh.shape["seq"], mesh.shape["head"]

    def body(hidden_states, feature_q, feature_k, value_w, window_q, window_k, norm_gain):
        rows, depth = hidden_states.shape
        heads = feature_q.shape[1] // FK
        full, width = value_w.shape
        ea, eb, mask = features(heads)
        feats = ea.shape[1]
        chunks = feats // CHUNK
        wire = BF16 if blocks <= 16 else F32
        dma, anywhere = pltpu.SemaphoreType.DMA, pl.BlockSpec(memory_space=pltpu.HBM)
        state = (chunks, HV, CHUNK)
        return pl.pallas_call(
            functools.partial(kernel, blocks, group, heads, wire),
            out_shape=jax.ShapeDtypeStruct((rows, width), BF16),
            in_specs=[anywhere] * 10,
            out_specs=pl.BlockSpec(memory_space=pltpu.VMEM),
            scratch_shapes=[
                pltpu.VMEM((group, rows, depth), BF16),
                pltpu.VMEM((heads * FK, full), BF16),
                pltpu.VMEM((heads * FK, full), BF16),
                pltpu.VMEM((full, width), BF16),
                pltpu.VMEM((full, width), BF16),
                pltpu.VMEM((full, width), BF16),
                pltpu.VMEM((width,), F32),
                pltpu.VMEM(ea.shape, BF16),
                pltpu.VMEM(eb.shape, BF16),
                pltpu.VMEM(mask.shape, F32),
                pltpu.VMEM((rows, LANES), F32),
                pltpu.VMEM((rows, LANES), F32),
                pltpu.VMEM((rows, width), F32),
                pltpu.VMEM((rows, width), F32),
                pltpu.VMEM((rows, width), F32),
                pltpu.VMEM((rows, width), BF16),
                pltpu.VMEM((rows, width), BF16),
                pltpu.VMEM((rows, width), BF16),
                pltpu.VMEM((WIN, 2 * width), BF16),
                pltpu.VMEM((WIN, 2 * width), BF16),
                pltpu.VMEM((rows, feats), BF16),
                pltpu.VMEM(state, F32),
                pltpu.VMEM(state, wire),
                pltpu.VMEM(state, wire),
                pltpu.VMEM(state, wire),
                pltpu.VMEM(state, wire),
                pltpu.VMEM((rows, width), F32),
                pltpu.VMEM((rows, width), F32),
                dma((10,)),
                dma((group - 1,)),
                dma((group - 1,)),
                dma,
                dma,
                dma((chunks,)),
                dma((chunks,)),
                dma((chunks,)),
                dma((chunks,)),
            ],
            compiler_params=pltpu.CompilerParams(
                collective_id=0, has_side_effects=True, vmem_limit_bytes=40 * 1024 * 1024
            ),
            name="based_layer",
        )(*(pltpu.with_memory_space_constraint(operand, pltpu.HBM) for operand in (
            hidden_states, feature_q.T, feature_k.T, value_w, window_q, window_k,
            norm_gain, jnp.asarray(ea, BF16), jnp.asarray(eb, BF16),
            jnp.asarray(mask, F32),
        )))

    return jax.shard_map(
        body,
        mesh=mesh,
        in_specs=(P("seq", "head"),) + (P(None, "head"),) * 5 + (P("head"),),
        out_specs=P("seq", "head"),
        check_vma=False,
    )
```

```python
import functools

import jax
import jax.numpy as jnp
import numpy as np
from jax import lax
from jax.experimental import pallas as pl
from jax.experimental.pallas import tpu as pltpu
from jax.sharding import PartitionSpec as P

FK = 16
HV = 64
WIN = 64
LANES = 128
CHUNK = 128
WIDE = 256
MESH = pl.DeviceIdType.MESH
F32 = jnp.float32
BF16 = jnp.bfloat16


def features(heads):
    upper, lower = np.triu_indices(FK)
    one = heads * FK
    left, right, owner, weight = [], [], [], []
    for head in range(heads):
        base = head * FK
        left += [one] + [base + i for i in range(FK)] + [base + i for i in upper]
        right += [one] + [one] * FK + [base + j for j in lower]
        owner += [head] * (1 + FK + len(upper))
        weight += [1.0] * (1 + FK) + [0.5 if i == j else 1.0 for i, j in zip(upper, lower)]
    count = len(left)
    width = -(-count // WIDE) * WIDE
    ea = np.zeros((2 * LANES, width), np.float32)
    eb = np.zeros((2 * LANES, width), np.float32)
    mask = np.zeros((-(-heads // 8) * 8, width), np.float32)
    for lane in range(count):
        ea[[left[lane], LANES + left[lane]], lane] = 1.0
        eb[[right[lane], LANES + right[lane]], lane] = 1.0
        mask[owner[lane], lane] = weight[lane]
    return ea, eb, mask


def pair_range(wide, heads):
    each = 1 + FK + FK * (FK + 1) // 2
    first = min(wide * WIDE // each, heads - 1)
    last = min(((wide + 1) * WIDE - 1) // each, heads - 1)
    return first // 2, last // 2 + 1


def dot(a, b):
    return jnp.dot(a, b, preferred_element_type=F32)


def dot_t(a, b):
    return lax.dot_general(a, b, (((1,), (1,)), ((), ())), preferred_element_type=F32)


def split(x):
    high = x.astype(BF16)
    return high, (x - high.astype(F32)).astype(BF16)


def kernel(blocks, group, heads, wire, hid, fq, fk, vw, wqw, wkw, gain, ea, eb, mask, out,
           hbuf, fq_v, fk_v, vw_v, wq_v, wk_v, gain_v, ea_v, eb_v, mask_v,
           q_acc, k_acc, v_acc, wq_acc, wk_acc, v_b, wq_b, wk_b, halo_out, halo_in,
           phi_q, local, y_out, y_in, z_out, z_in, lin, win,
           load_sem, g_send, g_recv, h_send, h_recv, y_send, y_recv, z_send, z_recv):
    s, h = lax.axis_index("seq"), lax.axis_index("head")
    rows, depth = hid.shape
    chunks = local.shape[0]
    pair, inner = s // 2, s % 2
    last_pair = blocks // 2 - 1
    pairs = heads // 2

    loads = [
        pltpu.make_async_copy(src, dst, load_sem.at[i])
        for i, (src, dst) in enumerate((
            (hid, hbuf.at[h]), (fk, fk_v), (vw, vw_v), (wkw, wk_v), (fq, fq_v), (wqw, wq_v),
            (ea, ea_v), (eb, eb_v), (mask, mask_v), (gain, gain_v),
        ))
    ]
    for load in loads:
        load.start()

    barrier = pltpu.get_barrier_semaphore()
    bits = []
    bit = group // 2
    while bit:
        bits.append(bit)
        bit //= 2

    def flip(value, by):
        return value + by - 2 * by * ((value // by) % 2)

    for by in bits:
        pl.semaphore_signal(barrier, inc=1, device_id=(s, flip(h, by)), device_id_type=MESH)
    expected = len(bits)
    for by in (1, -1, 2, -2):
        there = s + by
        valid = jnp.logical_and(there >= 0, there < blocks)

        @pl.when(valid)
        def _(there=there):
            pl.semaphore_signal(barrier, inc=1, device_id=(there, h), device_id_type=MESH)

        expected = expected + jnp.where(valid, 1, 0)

    lane = lax.broadcasted_iota(jnp.int32, (rows, LANES), 1)
    fill = jnp.where(lane >= heads * FK, FK**0.25, 0.0).astype(F32)
    q_acc[...] = fill
    k_acc[...] = fill
    pl.semaphore_wait(barrier, expected)
    loads[0].wait()

    moves = {}

    def send_block(index, owner, by):
        move = pltpu.make_async_remote_copy(
            src_ref=hbuf.at[owner], dst_ref=hbuf.at[owner],
            send_sem=g_send.at[index], recv_sem=g_recv.at[index],
            device_id=(s, flip(h, by)), device_id_type=MESH,
        )
        move.start()
        return move

    plan = []

    def spread(owner_flip, from_level):
        for level in range(from_level, len(bits)):
            plan.append((owner_flip, level))
            spread(owner_flip ^ bits[level], level + 1)

    spread(0, 0)
    arrives = {}
    for index, (own, level) in enumerate(plan):
        arrives[own ^ bits[level]] = index

    def owner_of(mask_bits):
        value = h
        for by in bits:
            if mask_bits & by:
                value = flip(value, by)
        return value

    def forward(block):
        for index, (own, level) in enumerate(plan):
            if own == block:
                moves[index] = send_block(index, owner_of(block), bits[level])

    def arrive(block):
        moves_index = arrives[block]
        moves[moves_index].wait_recv()

    def part(weight, owner):
        return weight[pl.ds(pl.multiple_of(owner * depth, depth), depth), :]

    def part_t(weight, owner):
        return weight[:, pl.ds(pl.multiple_of(owner * depth, depth), depth)]

    forward(0)
    sequence = sorted(range(1, group), key=lambda b: (b.bit_length(), b))
    main = ((v_acc, vw_v), (wk_acc, wk_v), (wq_acc, wq_v))
    small = ((k_acc, fk_v), (q_acc, fq_v))
    for load in loads[1:6]:
        load.wait()
    for position, block in enumerate([0] + sequence):
        if block:
            arrive(block)
            forward(block)
        owner = owner_of(block)
        tile = hbuf[owner]
        final = position == group - 1
        for acc, weight in small:
            if final and acc is q_acc:
                continue
            acc[:, : heads * FK] += dot_t(tile, part_t(weight, owner))
        for acc, weight in main:
            if final and acc is not v_acc:
                continue
            product = dot(tile, part(weight, owner))
            acc[...] = product if position == 0 else acc[...] + product
    last_tile, last_owner = tile, owner

    v_b[...] = v_acc[...].astype(BF16)
    for load in loads[6:]:
        load.wait()

    k_high, k_low = split(k_acc[...] * FK**-0.25)
    k_cat = jnp.concatenate([k_high, k_low], axis=1)
    v_turned = v_b[...].T
    exchange = []
    for wide in range(chunks * CHUNK // WIDE):
        lanes = slice(wide * WIDE, (wide + 1) * WIDE)
        phi_k = (dot(k_cat, ea_v[:, lanes]) * dot(k_cat, eb_v[:, lanes])).astype(BF16)
        p0, p1 = pair_range(wide, heads)
        full = dot(v_turned[p0 * LANES : p1 * LANES], phi_k)
        state = 0.0
        for head in range(2 * p0, 2 * p1):
            at = (head - 2 * p0) * HV
            state += full[at : at + HV] * mask_v[head : head + 1, lanes]
        for piece in range(WIDE // CHUNK):
            c = wide * (WIDE // CHUNK) + piece
            part_state = state[:, piece * CHUNK : (piece + 1) * CHUNK]
            local[c] = part_state
            y_out[c] = part_state.astype(wire)
            move = pltpu.make_async_remote_copy(
                src_ref=y_out.at[c], dst_ref=y_in.at[c],
                send_sem=y_send.at[c], recv_sem=y_recv.at[c],
                device_id=(flip(s, 1), h), device_id_type=MESH,
            )
            move.start()
            exchange.append(move)
    beyond = lax.rem(s + 2, blocks)
    chain = [
        pltpu.make_async_remote_copy(
            src_ref=z_out.at[c], dst_ref=z_in.at[c], send_sem=z_send.at[c], recv_sem=z_recv.at[c],
            device_id=(beyond, h), device_id_type=MESH,
        )
        for c in range(chunks)
    ]

    wk_b[...] = (wk_acc[...] + dot(last_tile, part(wk_v, last_owner))).astype(BF16)
    width = heads * HV
    halo_out[:, :width] = wk_b[rows - WIN :, :]
    halo_out[:, width:] = v_b[rows - WIN :, :]
    after = lax.rem(s + 1, blocks)
    halo = pltpu.make_async_remote_copy(
        src_ref=halo_out, dst_ref=halo_in, send_sem=h_send, recv_sem=h_recv,
        device_id=(after, h), device_id_type=MESH,
    )

    late = jnp.logical_and(pair == 0, inner == 1)

    @pl.when(jnp.logical_and(s < blocks - 1, jnp.logical_not(late)))
    def _():
        halo.start()

    wq_b[...] = (wq_acc[...] + dot(last_tile, part(wq_v, last_owner))).astype(BF16)
    low_win = lax.broadcasted_iota(jnp.int32, (WIN, LANES), 1) < HV
    row_w = lax.broadcasted_iota(jnp.int32, (2 * WIN, 2 * WIN), 0) % WIN
    col_w = lax.broadcasted_iota(jnp.int32, (2 * WIN, 2 * WIN), 1)
    seen = jnp.logical_and(col_w > row_w, col_w <= row_w + WIN)

    def window(p, block):
        ls = slice(p * LANES, (p + 1) * LANES)
        qs = wq_b[block * WIN : (block + 1) * WIN, ls]
        stacked = jnp.concatenate([jnp.where(low_win, qs, 0), jnp.where(low_win, 0, qs)], axis=0)
        valid = seen
        if block == 0:
            keys = jnp.concatenate([halo_in[:, ls], wk_b[:WIN, ls]], axis=0)
            vals = jnp.concatenate(
                [halo_in[:, width + p * LANES : width + (p + 1) * LANES], v_b[:WIN, ls]], axis=0
            )
            valid = jnp.logical_and(seen, jnp.logical_or(col_w >= WIN, s > 0))
        else:
            keys = wk_b[(block - 1) * WIN : (block + 1) * WIN, ls]
            vals = v_b[(block - 1) * WIN : (block + 1) * WIN, ls]
        logits = jnp.where(valid, dot_t(stacked, keys) * HV**-0.5, -1e30)
        expw = jnp.exp(logits - jnp.max(logits, axis=-1, keepdims=True))
        weights = (expw / jnp.sum(expw, axis=-1, keepdims=True)).astype(BF16)
        both = dot(weights, vals)
        win[block * WIN : (block + 1) * WIN, ls] = jnp.where(low_win, both[:WIN], both[WIN:])

    def windows():
        for p in range(pairs):
            for block in range(1, rows // WIN):
                window(p, block)

    pl.when(pair > 0)(windows)

    for c in range(chunks):
        exchange[c].wait_recv()

        @pl.when(pair == 0)
        def _(c=c):
            z_out[c] = (local[c] + y_in[c].astype(F32)).astype(wire)
            z_in[c] = jnp.zeros_like(z_in[c])

            @pl.when(pair < last_pair)
            def _():
                chain[c].start()

    @pl.when(jnp.logical_and(s < blocks - 1, late))
    def _():
        halo.start()

    def relay(c):
        chain[c].wait_recv()

        @pl.when(pair < last_pair)
        def _():
            z_out[c] = (z_in[c].astype(F32) + (local[c] + y_in[c].astype(F32))).astype(wire)
            chain[c].start()

    @pl.when(pair == 1)
    def _():
        for c in range(chunks):
            relay(c)

    pl.when(pair == 0)(windows)
    q_acc[:, : heads * FK] += dot_t(last_tile, part_t(fq_v, last_owner))
    q_high, q_low = split(q_acc[...] * FK**-0.25)
    q_cat = jnp.concatenate([q_high, q_low], axis=1)

    def features_q():
        for wide in range(chunks * CHUNK // WIDE):
            lanes = slice(wide * WIDE, (wide + 1) * WIDE)
            phi_q[:, lanes] = (dot(q_cat, ea_v[:, lanes]) * dot(q_cat, eb_v[:, lanes])).astype(BF16)

    k_twice = jnp.concatenate([k_high, k_high], axis=1)
    half = rows // 2
    lane_q = lax.broadcasted_iota(jnp.int32, (half, 2 * LANES), 1) % LANES // FK
    low_half = lax.broadcasted_iota(jnp.int32, (half, LANES), 1) < HV

    def intra(p, block):
        rs = slice(block * half, (block + 1) * half)
        keys = (block + 1) * half
        qs = q_cat[rs]
        stacked = jnp.concatenate(
            [jnp.where(lane_q == 2 * p, qs, 0), jnp.where(lane_q == 2 * p + 1, qs, 0)], axis=0
        )
        a = dot_t(stacked, k_twice[:keys]) + dot_t(stacked[:, :LANES], k_low[:keys])
        kern = 1.0 + a + 0.5 * a * a
        row = lax.broadcasted_iota(jnp.int32, a.shape, 0) % half + block * half
        col = lax.broadcasted_iota(jnp.int32, a.shape, 1)
        kern = jnp.where(row >= col, kern, 0.0).astype(BF16)
        both = dot(kern, v_b[:keys, p * LANES : (p + 1) * LANES])
        lin[rs, p * LANES : (p + 1) * LANES] = jnp.where(low_half, both[:half], both[half:])

    features_q()
    for p in range(pairs):
        for block in range(2):
            intra(p, block)

    @pl.when(s > 0)
    def _():
        halo.wait_recv()

    @pl.when(s == 0)
    def _():
        halo_in[...] = jnp.zeros_like(halo_in)

    for p in range(pairs):
        window(p, 0)

    mine = jnp.where(inner == 1, 1.0, 0.0).astype(F32)
    ones = jnp.where(
        lax.broadcasted_iota(jnp.int32, (2 * LANES, LANES), 0) % LANES // HV
        == lax.broadcasted_iota(jnp.int32, (2 * LANES, LANES), 1) // HV,
        1.0,
        0.0,
    ).astype(BF16)

    def finish(p):
        ls = slice(p * LANES, (p + 1) * LANES)
        linear = lin[:, ls]
        high, low = split(linear * linear)
        mean = dot(jnp.concatenate([high, low], axis=1), ones) * (1.0 / HV)
        normed = linear * lax.rsqrt(mean + 1e-05) * gain_v[ls].reshape(1, LANES)
        out[:, ls] = (normed + win[:, ls]).astype(BF16)

    finished = 0
    wides = chunks * CHUNK // WIDE
    for wide in range(wides):
        lanes = slice(wide * WIDE, (wide + 1) * WIDE)
        pieces = range(wide * (WIDE // CHUNK), (wide + 1) * (WIDE // CHUNK))

        @pl.when(pair > 1)
        def _(pieces=pieces):
            for c in pieces:
                relay(c)

        p0, p1 = pair_range(wide, heads)
        earlier = jnp.concatenate(
            [z_in[c].astype(F32) + mine * y_in[c].astype(F32) for c in pieces], axis=1
        )
        big = jnp.concatenate(
            [
                jnp.where(mask_v[head : head + 1, lanes] > 0, earlier, 0.0).astype(BF16)
                for head in range(2 * p0, 2 * p1)
            ],
            axis=0,
        )
        lin[:, p0 * LANES : p1 * LANES] += dot_t(phi_q[:, lanes], big)
        ready = pairs if wide + 1 == wides else pair_range(wide + 1, heads)[0]
        for p in range(finished, ready):
            finish(p)
        finished = max(finished, ready)

    for move in moves.values():
        move.wait_send()
    for move in exchange:
        move.wait_send()

    @pl.when(s < blocks - 1)
    def _():
        halo.wait_send()

    @pl.when(pair < last_pair)
    def _():
        for move in chain:
            move.wait_send()


def solution(mesh):
    blocks, group = mesh.shape["seq"], mesh.shape["head"]

    def body(hidden_states, feature_q, feature_k, value_w, window_q, window_k, norm_gain):
        rows, depth = hidden_states.shape
        heads = feature_q.shape[1] // FK
        full, width = value_w.shape
        ea, eb, mask = features(heads)
        feats = ea.shape[1]
        chunks = feats // CHUNK
        wire = BF16 if blocks <= 16 else F32
        dma, anywhere = pltpu.SemaphoreType.DMA, pl.BlockSpec(memory_space=pltpu.HBM)
        state = (chunks, HV, CHUNK)
        return pl.pallas_call(
            functools.partial(kernel, blocks, group, heads, wire),
            out_shape=jax.ShapeDtypeStruct((rows, width), BF16),
            in_specs=[anywhere] * 10,
            out_specs=pl.BlockSpec(memory_space=pltpu.VMEM),
            scratch_shapes=[
                pltpu.VMEM((group, rows, depth), BF16),
                pltpu.VMEM((heads * FK, full), BF16),
                pltpu.VMEM((heads * FK, full), BF16),
                pltpu.VMEM((full, width), BF16),
                pltpu.VMEM((full, width), BF16),
                pltpu.VMEM((full, width), BF16),
                pltpu.VMEM((width,), F32),
                pltpu.VMEM(ea.shape, BF16),
                pltpu.VMEM(eb.shape, BF16),
                pltpu.VMEM(mask.shape, F32),
                pltpu.VMEM((rows, LANES), F32),
                pltpu.VMEM((rows, LANES), F32),
                pltpu.VMEM((rows, width), F32),
                pltpu.VMEM((rows, width), F32),
                pltpu.VMEM((rows, width), F32),
                pltpu.VMEM((rows, width), BF16),
                pltpu.VMEM((rows, width), BF16),
                pltpu.VMEM((rows, width), BF16),
                pltpu.VMEM((WIN, 2 * width), BF16),
                pltpu.VMEM((WIN, 2 * width), BF16),
                pltpu.VMEM((rows, feats), BF16),
                pltpu.VMEM(state, F32),
                pltpu.VMEM(state, wire),
                pltpu.VMEM(state, wire),
                pltpu.VMEM(state, wire),
                pltpu.VMEM(state, wire),
                pltpu.VMEM((rows, width), F32),
                pltpu.VMEM((rows, width), F32),
                dma((10,)),
                dma((group - 1,)),
                dma((group - 1,)),
                dma,
                dma,
                dma((chunks,)),
                dma((chunks,)),
                dma((chunks,)),
                dma((chunks,)),
            ],
            compiler_params=pltpu.CompilerParams(
                collective_id=0, has_side_effects=True, vmem_limit_bytes=40 * 1024 * 1024
            ),
            name="based_layer",
        )(*(pltpu.with_memory_space_constraint(operand, pltpu.HBM) for operand in (
            hidden_states, feature_q.T, feature_k.T, value_w, window_q, window_k,
            norm_gain, jnp.asarray(ea, BF16), jnp.asarray(eb, BF16),
            jnp.asarray(mask, F32),
        )))

    return jax.shard_map(
        body,
        mesh=mesh,
        in_specs=(P("seq", "head"),) + (P(None, "head"),) * 5 + (P("head"),),
        out_specs=P("seq", "head"),
        check_vma=False,
    )
```

```python
import functools

import jax
import jax.numpy as jnp
import numpy as np
from jax import lax
from jax.experimental import pallas as pl
from jax.experimental.pallas import tpu as pltpu
from jax.sharding import PartitionSpec as P

FK = 16
HV = 64
WIN = 64
LANES = 128
CHUNK = 128
WIDE = 256
MESH = pl.DeviceIdType.MESH
F32 = jnp.float32
BF16 = jnp.bfloat16


def features(heads):
    upper, lower = np.triu_indices(FK)
    one = heads * FK
    left, right, owner, weight = [], [], [], []
    for head in range(heads):
        base = head * FK
        left += [one] + [base + i for i in range(FK)] + [base + i for i in upper]
        right += [one] + [one] * FK + [base + j for j in lower]
        owner += [head] * (1 + FK + len(upper))
        weight += [1.0] * (1 + FK) + [0.5 if i == j else 1.0 for i, j in zip(upper, lower)]
    count = len(left)
    width = -(-count // WIDE) * WIDE
    ea = np.zeros((2 * LANES, width), np.float32)
    eb = np.zeros((2 * LANES, width), np.float32)
    mask = np.zeros((-(-heads // 8) * 8, width), np.float32)
    for lane in range(count):
        ea[[left[lane], LANES + left[lane]], lane] = 1.0
        eb[[right[lane], LANES + right[lane]], lane] = 1.0
        mask[owner[lane], lane] = weight[lane]
    return ea, eb, mask


def pair_range(wide, heads):
    each = 1 + FK + FK * (FK + 1) // 2
    first = min(wide * WIDE // each, heads - 1)
    last = min(((wide + 1) * WIDE - 1) // each, heads - 1)
    return first // 2, last // 2 + 1


def dot(a, b):
    return jnp.dot(a, b, preferred_element_type=F32)


def dot_t(a, b):
    return lax.dot_general(a, b, (((1,), (1,)), ((), ())), preferred_element_type=F32)


def split(x):
    high = x.astype(BF16)
    return high, (x - high.astype(F32)).astype(BF16)


def kernel(blocks, group, heads, wire, hid, fq, fk, vw, wqw, wkw, gain, ea, eb, mask, out,
           hbuf, fq_v, fk_v, vw_v, wq_v, wk_v, gain_v, ea_v, eb_v, mask_v,
           q_acc, k_acc, v_acc, wq_acc, wk_acc, v_b, wq_b, wk_b, halo_out, halo_in,
           phi_q, local, y_out, y_in, z_out, z_in, lin, win,
           load_sem, g_send, g_recv, h_send, h_recv, y_send, y_recv, z_send, z_recv):
    s, h = lax.axis_index("seq"), lax.axis_index("head")
    rows, depth = hid.shape
    chunks = local.shape[0]
    pair, inner = s // 2, s % 2
    last_pair = blocks // 2 - 1
    pairs = heads // 2

    loads = [
        pltpu.make_async_copy(src, dst, load_sem.at[i])
        for i, (src, dst) in enumerate((
            (hid, hbuf.at[h]), (fk, fk_v), (vw, vw_v), (wkw, wk_v), (fq, fq_v), (wqw, wq_v),
            (ea, ea_v), (eb, eb_v), (mask, mask_v), (gain, gain_v),
        ))
    ]
    for load in loads:
        load.start()

    barrier = pltpu.get_barrier_semaphore()
    bits = []
    bit = group // 2
    while bit:
        bits.append(bit)
        bit //= 2

    def flip(value, by):
        return value + by - 2 * by * ((value // by) % 2)

    for by in bits:
        pl.semaphore_signal(barrier, inc=1, device_id=(s, flip(h, by)), device_id_type=MESH)
    expected = len(bits)
    for by in (1, -1, 2, -2):
        there = s + by
        valid = jnp.logical_and(there >= 0, there < blocks)

        @pl.when(valid)
        def _(there=there):
            pl.semaphore_signal(barrier, inc=1, device_id=(there, h), device_id_type=MESH)

        expected = expected + jnp.where(valid, 1, 0)

    lane = lax.broadcasted_iota(jnp.int32, (rows, LANES), 1)
    fill = jnp.where(lane >= heads * FK, FK**0.25, 0.0).astype(F32)
    q_acc[...] = fill
    k_acc[...] = fill
    pl.semaphore_wait(barrier, expected)
    loads[0].wait()

    moves = {}

    def send_block(index, owner, by):
        move = pltpu.make_async_remote_copy(
            src_ref=hbuf.at[owner], dst_ref=hbuf.at[owner],
            send_sem=g_send.at[index], recv_sem=g_recv.at[index],
            device_id=(s, flip(h, by)), device_id_type=MESH,
        )
        move.start()
        return move

    plan = []

    def spread(owner_flip, from_level):
        for level in range(from_level, len(bits)):
            plan.append((owner_flip, level))
            spread(owner_flip ^ bits[level], level + 1)

    spread(0, 0)
    arrives = {}
    for index, (own, level) in enumerate(plan):
        arrives[own ^ bits[level]] = index

    def owner_of(mask_bits):
        value = h
        for by in bits:
            if mask_bits & by:
                value = flip(value, by)
        return value

    def forward(block):
        for index, (own, level) in enumerate(plan):
            if own == block:
                moves[index] = send_block(index, owner_of(block), bits[level])

    def arrive(block):
        moves_index = arrives[block]
        moves[moves_index].wait_recv()

    def part(weight, owner):
        return weight[pl.ds(pl.multiple_of(owner * depth, depth), depth), :]

    def part_t(weight, owner):
        return weight[:, pl.ds(pl.multiple_of(owner * depth, depth), depth)]

    forward(0)
    sequence = sorted(range(1, group), key=lambda b: (b.bit_length(), b))
    main = ((v_acc, vw_v), (wk_acc, wk_v), (wq_acc, wq_v))
    small = ((k_acc, fk_v), (q_acc, fq_v))
    for load in loads[1:6]:
        load.wait()
    for position, block in enumerate([0] + sequence):
        if block:
            arrive(block)
            forward(block)
        owner = owner_of(block)
        tile = hbuf[owner]
        final = position == group - 1
        for acc, weight in small:
            if final and acc is q_acc:
                continue
            acc[:, : heads * FK] += dot_t(tile, part_t(weight, owner))
        for acc, weight in main:
            if final and acc is not v_acc:
                continue
            product = dot(tile, part(weight, owner))
            acc[...] = product if position == 0 else acc[...] + product
    last_tile, last_owner = tile, owner

    v_b[...] = v_acc[...].astype(BF16)
    width = heads * HV
    after = lax.rem(s + 1, blocks)
    halo = pltpu.make_async_remote_copy(
        src_ref=halo_out, dst_ref=halo_in, send_sem=h_send, recv_sem=h_recv,
        device_id=(after, h), device_id_type=MESH,
    )

    def window_keys():
        wk_b[...] = (wk_acc[...] + dot(last_tile, part(wk_v, last_owner))).astype(BF16)
        halo_out[:, :width] = wk_b[rows - WIN :, :]
        halo_out[:, width:] = v_b[rows - WIN :, :]

    @pl.when(pair > 0)
    def _():
        window_keys()

        @pl.when(s < blocks - 1)
        def _():
            halo.start()

    for load in loads[6:]:
        load.wait()

    k_high, k_low = split(k_acc[...] * FK**-0.25)
    k_cat = jnp.concatenate([k_high, k_low], axis=1)
    v_turned = v_b[...].T
    exchange = []
    for wide in range(chunks * CHUNK // WIDE):
        lanes = slice(wide * WIDE, (wide + 1) * WIDE)
        phi_k = (dot(k_cat, ea_v[:, lanes]) * dot(k_cat, eb_v[:, lanes])).astype(BF16)
        p0, p1 = pair_range(wide, heads)
        full = dot(v_turned[p0 * LANES : p1 * LANES], phi_k)
        state = 0.0
        for head in range(2 * p0, 2 * p1):
            at = (head - 2 * p0) * HV
            state += full[at : at + HV] * mask_v[head : head + 1, lanes]
        for piece in range(WIDE // CHUNK):
            c = wide * (WIDE // CHUNK) + piece
            part_state = state[:, piece * CHUNK : (piece + 1) * CHUNK]
            local[c] = part_state
            y_out[c] = part_state.astype(wire)
            move = pltpu.make_async_remote_copy(
                src_ref=y_out.at[c], dst_ref=y_in.at[c],
                send_sem=y_send.at[c], recv_sem=y_recv.at[c],
                device_id=(flip(s, 1), h), device_id_type=MESH,
            )
            move.start()
            exchange.append(move)
    beyond = lax.rem(s + 2, blocks)
    chain = [
        pltpu.make_async_remote_copy(
            src_ref=z_out.at[c], dst_ref=z_in.at[c], send_sem=z_send.at[c], recv_sem=z_recv.at[c],
            device_id=(beyond, h), device_id_type=MESH,
        )
        for c in range(chunks)
    ]

    @pl.when(pair == 0)
    def _():
        window_keys()

        @pl.when(jnp.logical_and(s < blocks - 1, inner == 0))
        def _():
            halo.start()

    wq_b[...] = (wq_acc[...] + dot(last_tile, part(wq_v, last_owner))).astype(BF16)
    low_win = lax.broadcasted_iota(jnp.int32, (WIN, LANES), 1) < HV
    row_w = lax.broadcasted_iota(jnp.int32, (2 * WIN, 2 * WIN), 0) % WIN
    col_w = lax.broadcasted_iota(jnp.int32, (2 * WIN, 2 * WIN), 1)
    seen = jnp.logical_and(col_w > row_w, col_w <= row_w + WIN)

    def window(p, block):
        ls = slice(p * LANES, (p + 1) * LANES)
        qs = wq_b[block * WIN : (block + 1) * WIN, ls]
        stacked = jnp.concatenate([jnp.where(low_win, qs, 0), jnp.where(low_win, 0, qs)], axis=0)
        valid = seen
        if block == 0:
            keys = jnp.concatenate([halo_in[:, ls], wk_b[:WIN, ls]], axis=0)
            vals = jnp.concatenate(
                [halo_in[:, width + p * LANES : width + (p + 1) * LANES], v_b[:WIN, ls]], axis=0
            )
            valid = jnp.logical_and(seen, jnp.logical_or(col_w >= WIN, s > 0))
        else:
            keys = wk_b[(block - 1) * WIN : (block + 1) * WIN, ls]
            vals = v_b[(block - 1) * WIN : (block + 1) * WIN, ls]
        logits = jnp.where(valid, dot_t(stacked, keys) * HV**-0.5, -1e30)
        expw = jnp.exp(logits - jnp.max(logits, axis=-1, keepdims=True))
        weights = (expw / jnp.sum(expw, axis=-1, keepdims=True)).astype(BF16)
        both = dot(weights, vals)
        win[block * WIN : (block + 1) * WIN, ls] = jnp.where(low_win, both[:WIN], both[WIN:])

    spots = [(p, block) for p in range(pairs) for block in range(1, rows // WIN)]

    def rest():
        q_acc[:, : heads * FK] += dot_t(last_tile, part_t(fq_v, last_owner))
        q_high, q_low = split(q_acc[...] * FK**-0.25)
        q_cat = jnp.concatenate([q_high, q_low], axis=1)

        def features_q():
            for wide in range(chunks * CHUNK // WIDE):
                lanes = slice(wide * WIDE, (wide + 1) * WIDE)
                phi_q[:, lanes] = (dot(q_cat, ea_v[:, lanes]) * dot(q_cat, eb_v[:, lanes])).astype(BF16)

        k_twice = jnp.concatenate([k_high, k_high], axis=1)
        half = rows // 2
        lane_q = lax.broadcasted_iota(jnp.int32, (half, 2 * LANES), 1) % LANES // FK
        low_half = lax.broadcasted_iota(jnp.int32, (half, LANES), 1) < HV

        def intra(p, block):
            rs = slice(block * half, (block + 1) * half)
            keys = (block + 1) * half
            qs = q_cat[rs]
            stacked = jnp.concatenate(
                [jnp.where(lane_q == 2 * p, qs, 0), jnp.where(lane_q == 2 * p + 1, qs, 0)], axis=0
            )
            a = dot_t(stacked, k_twice[:keys]) + dot_t(stacked[:, :LANES], k_low[:keys])
            kern = 1.0 + a + 0.5 * a * a
            row = lax.broadcasted_iota(jnp.int32, a.shape, 0) % half + block * half
            col = lax.broadcasted_iota(jnp.int32, a.shape, 1)
            kern = jnp.where(row >= col, kern, 0.0).astype(BF16)
            both = dot(kern, v_b[:keys, p * LANES : (p + 1) * LANES])
            lin[rs, p * LANES : (p + 1) * LANES] = jnp.where(low_half, both[:half], both[half:])

        features_q()
        for p in range(pairs):
            for block in range(2):
                intra(p, block)

    def relay(c):
        exchange[c].wait_recv()
        chain[c].wait_recv()

        @pl.when(pair < last_pair)
        def _():
            z_out[c] = (z_in[c].astype(F32) + (local[c] + y_in[c].astype(F32))).astype(wire)
            chain[c].start()

    @pl.when(pair == 0)
    def _():
        for c in range(chunks):
            exchange[c].wait_recv()
            z_out[c] = (local[c] + y_in[c].astype(F32)).astype(wire)
            z_in[c] = jnp.zeros_like(z_in[c])

            @pl.when(pair < last_pair)
            def _(c=c):
                chain[c].start()

            for spot in spots[c :: chunks]:
                window(*spot)

        @pl.when(jnp.logical_and(s < blocks - 1, inner == 1))
        def _():
            halo.start()

    pl.when(pair > 0)(rest)

    @pl.when(pair > 1)
    def _():
        for spot in spots:
            window(*spot)

    @pl.when(pair == 1)
    def _():
        for spot in spots[:2]:
            window(*spot)
        for c in range(chunks):
            relay(c)
            for spot in spots[2 + c :: chunks]:
                window(*spot)

    pl.when(pair == 0)(rest)

    @pl.when(s > 0)
    def _():
        halo.wait_recv()

    @pl.when(s == 0)
    def _():
        halo_in[...] = jnp.zeros_like(halo_in)

    for p in range(pairs):
        window(p, 0)

    mine = jnp.where(inner == 1, 1.0, 0.0).astype(F32)
    ones = jnp.where(
        lax.broadcasted_iota(jnp.int32, (2 * LANES, LANES), 0) % LANES // HV
        == lax.broadcasted_iota(jnp.int32, (2 * LANES, LANES), 1) // HV,
        1.0,
        0.0,
    ).astype(BF16)

    def finish(p):
        ls = slice(p * LANES, (p + 1) * LANES)
        linear = lin[:, ls]
        high, low = split(linear * linear)
        mean = dot(jnp.concatenate([high, low], axis=1), ones) * (1.0 / HV)
        normed = linear * lax.rsqrt(mean + 1e-05) * gain_v[ls].reshape(1, LANES)
        out[:, ls] = (normed + win[:, ls]).astype(BF16)

    finished = 0
    wides = chunks * CHUNK // WIDE
    for wide in range(wides):
        lanes = slice(wide * WIDE, (wide + 1) * WIDE)
        pieces = range(wide * (WIDE // CHUNK), (wide + 1) * (WIDE // CHUNK))

        @pl.when(pair > 1)
        def _(pieces=pieces):
            for c in pieces:
                relay(c)

        p0, p1 = pair_range(wide, heads)
        earlier = jnp.concatenate(
            [z_in[c].astype(F32) + mine * y_in[c].astype(F32) for c in pieces], axis=1
        )
        big = jnp.concatenate(
            [
                jnp.where(mask_v[head : head + 1, lanes] > 0, earlier, 0.0).astype(BF16)
                for head in range(2 * p0, 2 * p1)
            ],
            axis=0,
        )
        lin[:, p0 * LANES : p1 * LANES] += dot_t(phi_q[:, lanes], big)
        ready = pairs if wide + 1 == wides else pair_range(wide + 1, heads)[0]
        for p in range(finished, ready):
            finish(p)
        finished = max(finished, ready)

    for move in moves.values():
        move.wait_send()
    for move in exchange:
        move.wait_send()

    @pl.when(s < blocks - 1)
    def _():
        halo.wait_send()

    @pl.when(pair < last_pair)
    def _():
        for move in chain:
            move.wait_send()


def solution(mesh):
    blocks, group = mesh.shape["seq"], mesh.shape["head"]

    def body(hidden_states, feature_q, feature_k, value_w, window_q, window_k, norm_gain):
        rows, depth = hidden_states.shape
        heads = feature_q.shape[1] // FK
        full, width = value_w.shape
        ea, eb, mask = features(heads)
        feats = ea.shape[1]
        chunks = feats // CHUNK
        wire = BF16 if blocks <= 16 else F32
        dma, anywhere = pltpu.SemaphoreType.DMA, pl.BlockSpec(memory_space=pltpu.HBM)
        state = (chunks, HV, CHUNK)
        return pl.pallas_call(
            functools.partial(kernel, blocks, group, heads, wire),
            out_shape=jax.ShapeDtypeStruct((rows, width), BF16),
            in_specs=[anywhere] * 10,
            out_specs=pl.BlockSpec(memory_space=pltpu.VMEM),
            scratch_shapes=[
                pltpu.VMEM((group, rows, depth), BF16),
                pltpu.VMEM((heads * FK, full), BF16),
                pltpu.VMEM((heads * FK, full), BF16),
                pltpu.VMEM((full, width), BF16),
                pltpu.VMEM((full, width), BF16),
                pltpu.VMEM((full, width), BF16),
                pltpu.VMEM((width,), F32),
                pltpu.VMEM(ea.shape, BF16),
                pltpu.VMEM(eb.shape, BF16),
                pltpu.VMEM(mask.shape, F32),
                pltpu.VMEM((rows, LANES), F32),
                pltpu.VMEM((rows, LANES), F32),
                pltpu.VMEM((rows, width), F32),
                pltpu.VMEM((rows, width), F32),
                pltpu.VMEM((rows, width), F32),
                pltpu.VMEM((rows, width), BF16),
                pltpu.VMEM((rows, width), BF16),
                pltpu.VMEM((rows, width), BF16),
                pltpu.VMEM((WIN, 2 * width), BF16),
                pltpu.VMEM((WIN, 2 * width), BF16),
                pltpu.VMEM((rows, feats), BF16),
                pltpu.VMEM(state, F32),
                pltpu.VMEM(state, wire),
                pltpu.VMEM(state, wire),
                pltpu.VMEM(state, wire),
                pltpu.VMEM(state, wire),
                pltpu.VMEM((rows, width), F32),
                pltpu.VMEM((rows, width), F32),
                dma((10,)),
                dma((group - 1,)),
                dma((group - 1,)),
                dma,
                dma,
                dma((chunks,)),
                dma((chunks,)),
                dma((chunks,)),
                dma((chunks,)),
            ],
            compiler_params=pltpu.CompilerParams(
                collective_id=0, has_side_effects=True, vmem_limit_bytes=40 * 1024 * 1024
            ),
            name="based_layer",
        )(*(pltpu.with_memory_space_constraint(operand, pltpu.HBM) for operand in (
            hidden_states, feature_q.T, feature_k.T, value_w, window_q, window_k,
            norm_gain, jnp.asarray(ea, BF16), jnp.asarray(eb, BF16),
            jnp.asarray(mask, F32),
        )))

    return jax.shard_map(
        body,
        mesh=mesh,
        in_specs=(P("seq", "head"),) + (P(None, "head"),) * 5 + (P("head"),),
        out_specs=P("seq", "head"),
        check_vma=False,
    )
```
